8 devices in a mesh: dp: 2 (over y, z), tp: 4 (over x, core).
Axes of the slice: x: 2, y: 2, z: 1, core: 2. Of those that a mesh axis runs over, the one named last changes fastest.
Arguments:
- x: bfloat16 [8, 512, 5120], P('dp'), parts along dimension 0
- gain_a: bfloat16 [5120], replicated
- wq: bfloat16 [5120, 5120], P(None, 'tp')
- wk: bfloat16 [5120, 5120], P(None, 'tp')
- wv: bfloat16 [5120, 5120], P(None, 'tp')
- wo: bfloat16 [5120, 5120], P('tp')
- gain_m: bfloat16 [5120], replicated
- w_gate: bfloat16 [5120, 13824], P(None, 'tp')
- w_up: bfloat16 [5120, 13824], P(None, 'tp')
- w_down: bfloat16 [13824, 5120], P('tp')
Outputs:
- output: bfloat16 [8, 512, 5120], P('dp'), parts along dimension 0
There are 2 independent parts. The reference program is written for one: setup_inputs(seed, part) draws one part's arguments, and reference() takes and returns one part's arrays. A program takes and returns all parts, laid end to end along the dimension named above; an argument that names none is the same for every part.
All inputs are finite; a program needn't handle non-finite values.
Results may differ from the reference program's by a relative error of at most 0.017.
Values are sent between devices in bfloat16 or wider.
A program may use at most 2 GiB of HBM per device.

```python
import jax
import jax.numpy as jnp
from jax import lax

SEQUENCES = 4
TOKENS = 512
D = 5120
HEADS = 40
KV_HEADS = 40
HEAD = 128
FF = 13824
THETA = 10000


def setup_inputs(seed: int = 0, part: int = 0) -> dict:
    kx, ka, km, kq, kk, kv, ko, kg, ku, kd = jax.random.split(jax.random.key(seed), 10)

    def weights(key, rows, columns):
        return jax.random.normal(key, (rows, columns), jnp.float32) * rows**-0.5

    drawn = {
        "x": jax.random.normal(jax.random.fold_in(kx, part), (SEQUENCES, TOKENS, D), jnp.float32),
        "gain_a": 1 + 0.1 * jax.random.normal(ka, (D,), jnp.float32),
        "wq": 2 * weights(kq, D, HEADS * HEAD),
        "wk": 2 * weights(kk, D, KV_HEADS * HEAD),
        "wv": 4 * weights(kv, D, KV_HEADS * HEAD),
        "wo": weights(ko, HEADS * HEAD, D),
        "gain_m": 1 + 0.1 * jax.random.normal(km, (D,), jnp.float32),
        "w_gate": weights(kg, D, FF),
        "w_up": weights(ku, D, FF),
        "w_down": 3 * weights(kd, FF, D),
    }
    return {k: v.astype(jnp.bfloat16) for k, v in drawn.items()}


def normed(x, gain):
    wide = x.astype(jnp.float32)
    scale = lax.rsqrt(jnp.mean(wide * wide, -1, keepdims=True) + 1e-6)
    return (wide * scale * gain.astype(jnp.float32)).astype(jnp.bfloat16)


def turned(t, place, theta):
    half = t.shape[-1] // 2
    angle = place.astype(jnp.float32)[:, None] * theta ** (-jnp.arange(half, dtype=jnp.float32) / half)
    cos, sin = jnp.cos(angle)[:, None], jnp.sin(angle)[:, None]
    a, b = t[..., :half].astype(jnp.float32), t[..., half:].astype(jnp.float32)
    return jnp.concatenate([a * cos - b * sin, b * cos + a * sin], -1).astype(jnp.bfloat16)


def matmul(a, w):
    return jnp.dot(a, w, preferred_element_type=jnp.float32).astype(jnp.bfloat16)


def einsum(form, a, b):
    return jnp.einsum(form, a.astype(jnp.float32), b.astype(jnp.float32))


def attention(q, k, v):
    scores = einsum("tgsd,ugd->gstu", q, k) * q.shape[-1] ** -0.5
    token = jnp.arange(q.shape[0])
    scores = jnp.where(token[:, None] >= token, scores, -jnp.inf)
    weights = jax.nn.softmax(scores, -1).astype(jnp.bfloat16)
    return einsum("gstu,ugd->tgsd", weights, v).astype(jnp.bfloat16)


def one(x, gain_a, wq, wk, wv, wo, gain_m, w_gate, w_up, w_down):
    rows = x.shape[0]
    a, place = normed(x, gain_a), jnp.arange(rows)
    k = turned(matmul(a, wk).reshape(rows, -1, HEAD), place, THETA)
    q = turned(matmul(a, wq).reshape(rows, -1, HEAD), place, THETA).reshape(rows, k.shape[1], -1, HEAD)
    v = matmul(a, wv).reshape(rows, -1, HEAD)
    seen = attention(q, k, v).reshape(rows, -1)
    h = (x.astype(jnp.float32) + jnp.dot(seen, wo, preferred_element_type=jnp.float32)).astype(jnp.bfloat16)
    b = normed(h, gain_m)
    gate = jnp.dot(b, w_gate, preferred_element_type=jnp.float32)
    up = jnp.dot(b, w_up, preferred_element_type=jnp.float32)
    hidden = (jax.nn.silu(gate) * up).astype(jnp.bfloat16)
    return (h.astype(jnp.float32) + jnp.dot(hidden, w_down, preferred_element_type=jnp.float32)).astype(jnp.bfloat16)


def reference(x, gain_a, wq, wk, wv, wo, gain_m, w_gate, w_up, w_down):
    return lax.map(lambda sequence: one(sequence, gain_a, wq, wk, wv, wo, gain_m, w_gate, w_up, w_down), x)
```

```python
import functools

import jax
import jax.numpy as jnp
from jax import lax
from jax.experimental import pallas as pl
from jax.experimental.pallas import tpu as pltpu
from jax.sharding import PartitionSpec as P

HEAD = 128
THETA = 10000
LOG2E = 1.4426950408889634
MESH = pl.DeviceIdType.MESH
BF, F32 = jnp.bfloat16, jnp.float32
VMEM = 60 * 2**20
CORES = [(0, 1), (1, 0), (2, 3), (3, 2)]
CHIPS = [(0, 2), (2, 0), (1, 3), (3, 1)]
ANY = pl.BlockSpec(memory_space=pl.ANY)


def dot(a, b):
    return jnp.dot(a, b, preferred_element_type=F32)


def core():
    return lax.rem(lax.axis_index("tp"), 2)


def start_greeting():
    pl.semaphore_signal(pltpu.get_barrier_semaphore(), inc=1, device_id=partner(), device_id_type=MESH)


def end_greeting():
    pl.semaphore_wait(pltpu.get_barrier_semaphore(), 1)


def partner():
    me = lax.axis_index("tp")
    return lax.axis_index("dp"), me + 1 - 2 * lax.rem(me, 2)


def sending(send_s, recv_s, ssem, rsem, j):
    return pltpu.make_async_remote_copy(
        src_ref=send_s.at[j], dst_ref=recv_s.at[j], send_sem=ssem.at[j], recv_sem=rsem.at[j], device_id=partner(), device_id_type=MESH
    )


def block_column(j, n):
    c = core()
    return jnp.where(j < n, (1 - c) * n + j, c * n + j - n)


def project(lhs_s, w_hbm, w_s, wsem, out_hbm, out_s, osem, send_s, recv_s, ssem, rsem, n):
    bn = w_s.shape[2]

    def theirs(j, _):
        slot = lax.rem(j, 2)
        fetch(w_hbm, w_s, wsem, block_column(j, n), slot, bn).wait()
        send_s[j] = dot(lhs_s[...], w_s[slot]).astype(BF)
        sending(send_s, recv_s, ssem, rsem, j).start()
        fetch(w_hbm, w_s, wsem, block_column(j + 2, n), slot, bn).start()
        return 0

    def mine(j, _):
        slot = lax.rem(j + n, 2)
        fetch(w_hbm, w_s, wsem, block_column(j + n, n), slot, bn).wait()
        total = dot(lhs_s[...], w_s[slot])

        @pl.when(j + 2 < n)
        def _():
            fetch(w_hbm, w_s, wsem, block_column(j + n + 2, n), slot, bn).start()

        sending(send_s, recv_s, ssem, rsem, j).wait_recv()
        side = lax.rem(j, 2)

        @pl.when(j >= 2)
        def _():
            give(out_s, out_hbm, osem, j - 2, side, bn).wait()

        out_s[side] = (total + recv_s[j].astype(F32)).astype(BF)
        give(out_s, out_hbm, osem, j, side, bn).start()
        return 0

    lax.fori_loop(0, n, theirs, 0)
    lax.fori_loop(0, n, mine, 0)
    for j in range(n):
        sending(send_s, recv_s, ssem, rsem, j).wait_send()
    for j in range(max(n - 2, 0), n):
        give(out_s, out_hbm, osem, j, j % 2, bn).wait()


def fetch(hbm, vmem, sem, block, slot, bn):
    return pltpu.make_async_copy(hbm.at[:, pl.ds(pl.multiple_of(block * bn, bn), bn)], vmem.at[slot], sem.at[slot])


def give(vmem, hbm, sem, block, slot, bn):
    return pltpu.make_async_copy(vmem.at[slot], hbm.at[:, pl.ds(pl.multiple_of(block * bn, bn), bn)], sem.at[slot])


def fetch_side_by_side(refs, vmem, sem, block, slot, wide):
    at = pl.ds(pl.multiple_of(block * wide, HEAD), wide)
    return [pltpu.make_async_copy(r.at[:, at], vmem.at[slot, :, k * wide : (k + 1) * wide], sem.at[slot, k]) for k, r in enumerate(refs)]


class Ride:
    def __init__(self, terms, bufs, mine, theirs, sems):
        self.loads = [pltpu.make_async_copy(t, b, sems.at[k]) for k, (t, b) in enumerate(zip(terms, bufs))]
        self.bufs = bufs
        self.keep = pltpu.make_async_copy(bufs[2], mine, sems.at[3])
        self.send = pltpu.make_async_remote_copy(
            src_ref=bufs[2], dst_ref=theirs, send_sem=sems.at[4], recv_sem=sems.at[5], device_id=partner(), device_id_type=MESH
        )

    def start(self):
        for copy in self.loads:
            copy.start()

    def work(self, step=16):
        for copy in self.loads:
            copy.wait()
        base, one, two = self.bufs

        def body(r, _):
            at = pl.ds(pl.multiple_of(r * step, step), step)
            two[at, :] = (base[at, :].astype(F32) + (one[at, :].astype(F32) + two[at, :].astype(F32))).astype(BF)
            return 0

        lax.fori_loop(0, two.shape[0] // step, body, 0, unroll=2)
        self.keep.start()
        self.send.start()

    def end(self):
        self.keep.wait()
        self.send.wait()


def norm_rows(parts, gains, out_ref, places, rows, width, step=16):
    def body(r, _):
        at = pl.ds(pl.multiple_of(r * step, step), step)
        wide = [p[at, :].astype(F32) for p in parts]
        total = sum(jnp.sum(w * w, -1, keepdims=True) for w in wide)
        scale = lax.rsqrt(total * (1.0 / width) + 1e-6)
        for w, g, place in zip(wide, gains, places):
            out_ref[at, pl.ds(place, w.shape[1])] = (w * scale * g()).astype(BF)
        return 0

    lax.fori_loop(0, rows // step, body, 0, unroll=4)


def attend_kernel(x_hbm, gain_ref, cos_ref, sin_ref, wq, wk, wv, wo, dep, *rest, s, n, riding):
    given, rest = (rest[:3], rest[3:]) if riding else ((), rest)
    (out_hbm, half_hbm), rest = rest[:2], rest[2:]
    made, rest = (rest[:2], rest[2:]) if riding else ((), rest)
    x_s, a_s, w_s, qkv_s, seen_s, wo_s, out_s, send_s, recv_s, xsem, wsem, wosem, osem, ssem, rsem, *rest = rest
    rows, width = x_s.shape
    half = width // 2
    own, wide = seen_s.shape[1], w_s.shape[2] // 3
    steps, bq = own // wide, rows // 2
    start_greeting()
    states = pltpu.make_async_copy(x_hbm.at[pl.ds(s * rows, rows)], x_s, xsem.at[0])
    states.start()
    weights = lambda i, slot: fetch_side_by_side([wq, wk, wv], w_s, wsem, i, slot, wide)
    for copy in weights(0, 0):
        copy.start()
    states.wait()
    keep = pltpu.make_async_copy(x_s.at[:, pl.ds(pl.multiple_of(core() * half, half), half)], half_hbm, xsem.at[1])
    keep.start()
    for copy in weights(1, 1):
        copy.start()
    norm_rows([x_s], [lambda: gain_ref[...].astype(F32)], a_s, [0], rows, width)
    keep.wait()
    end_greeting()
    ride = Ride(given, [x_s.at[:, :half], x_s.at[:, half:], rest[0]], *made, rest[1]) if riding else None

    def heads(i, slot):
        for copy in weights(i, slot):
            copy.wait()
        found = dot(a_s[...], w_s[slot])
        cos, sin = cos_ref[...], sin_ref[...]
        for k in range(3 * wide // HEAD):
            cols = slice(k * HEAD, (k + 1) * HEAD)
            t = found[:, cols].astype(BF)
            if k < 2 * wide // HEAD:
                t = t.astype(F32)
                t = (t * cos + pltpu.roll(t, HEAD // 2, 1) * sin).astype(BF)
            qkv_s[slot, :, cols] = t

    def attention(i, slot):
        e = HEAD**-0.5 * LOG2E
        hidden = lax.broadcasted_iota(jnp.int32, (bq, bq), 0) < lax.broadcasted_iota(jnp.int32, (bq, bq), 1)
        pieces = [(h, b) for h in range(wide // HEAD) for b in range(rows // bq)]
        part = lambda what, h: slice(what * wide + h * HEAD, what * wide + (h + 1) * HEAD)
        scores = []
        for h, b in pieces:
            q, k = qkv_s[slot, b * bq : (b + 1) * bq, part(0, h)], qkv_s[slot, : (b + 1) * bq, part(1, h)]
            scores.append(lax.dot_general(q, k, (((1,), (1,)), ((), ())), preferred_element_type=F32))
        weights = []
        for (h, b), t in zip(pieces, scores):
            last = jnp.where(hidden, -1e30, t[:, b * bq :])
            t = last if b == 0 else jnp.concatenate([t[:, : b * bq], last], 1)
            p = jnp.exp2((t - t.max(-1, keepdims=True)) * e)
            weights.append((p.astype(BF), p.sum(-1, keepdims=True)))
        for (h, b), (p, total) in zip(pieces, weights):
            o = dot(p, qkv_s[slot, : (b + 1) * bq, part(2, h)]) / total
            seen_s[b * bq : (b + 1) * bq, pl.ds(pl.multiple_of(i * wide + h * HEAD, HEAD), HEAD)] = o.astype(BF)

    def body(i, _):
        slot = lax.rem(i, 2)
        heads(i, slot)

        @pl.when(i + 2 < steps)
        def _():
            for copy in weights(i + 2, slot):
                copy.start()

        @pl.when(i >= steps - 2)
        def _():
            j = i - steps + 2
            fetch(wo, wo_s, wosem, block_column(j, n), j, wo_s.shape[2]).start()

        if riding:
            pl.when(i == 0)(ride.start)
            pl.when(i == 3)(ride.work)
        attention(i, slot)
        return 0

    lax.fori_loop(0, steps, body, 0)
    project(seen_s, wo, wo_s, wosem, out_hbm, out_s, osem, send_s, recv_s, ssem, rsem, n)
    if riding:
        ride.end()


def attend_half(x, s, rows, gain, cos, sin, wq, wk, wv, wo, dep, ride=(), wide=256, n=2):
    width, own = wq.shape
    bn = width // 2 // n
    half = jax.ShapeDtypeStruct((rows, width // 2), BF)
    whole = pl.BlockSpec(memory_space=pltpu.VMEM)
    return pl.pallas_call(
        functools.partial(attend_kernel, s=s, n=n, riding=bool(ride)),
        in_specs=[ANY, whole, whole, whole, ANY, ANY, ANY, ANY, ANY, *[ANY] * len(ride)],
        out_specs=[ANY] * (4 if ride else 2),
        out_shape=[half] * (4 if ride else 2),
        scratch_shapes=[pltpu.VMEM((rows, width), BF), pltpu.VMEM((rows, width), BF), pltpu.VMEM((2, width, 3 * wide), BF), pltpu.VMEM((2, rows, 3 * wide), BF),
                        pltpu.VMEM((rows, own), BF), pltpu.VMEM((2, own, bn), BF), pltpu.VMEM((2, rows, bn), BF),
                        pltpu.VMEM((n, rows, bn), BF), pltpu.VMEM((n, rows, bn), BF), pltpu.SemaphoreType.DMA((2,)), pltpu.SemaphoreType.DMA((2, 3)),
                        pltpu.SemaphoreType.DMA((2,)), pltpu.SemaphoreType.DMA((2,)), pltpu.SemaphoreType.DMA((n,)), pltpu.SemaphoreType.DMA((n,)),
                        *([pltpu.VMEM((rows, width // 2), BF), pltpu.SemaphoreType.DMA((6,))] if ride else [])],
        compiler_params=pltpu.CompilerParams(vmem_limit_bytes=VMEM, collective_id=s, has_side_effects=True),
        cost_estimate=pl.CostEstimate(flops=8 * rows * width * own, bytes_accessed=8 * width * own, transcendentals=0),
        name="attend_half",
    )(x, gain, cos, sin, wq, wk, wv, wo, dep, *ride)


def mlp_kernel(hm, ht, gain_ref, wg, wu, wd, dep, *rest, first, n, riding):
    given, rest = (rest[:3], rest[3:]) if riding else ((), rest)
    out_hbm, *rest = rest
    made, rest = (rest[:2], rest[2:]) if riding else ((), rest)
    h_s, b_s, w_s, hid_s, wd_s, out_s, send_s, recv_s, hsem, wsem, wdsem, osem, ssem, rsem, *rest = rest
    rows, half = h_s.shape[1:]
    own, wide = hid_s.shape[1], w_s.shape[2] // 2
    steps = own // wide
    start_greeting()
    states = [pltpu.make_async_copy(r.at[pl.ds(first, rows)], h_s.at[k], hsem.at[k]) for k, r in enumerate((hm, ht))]
    for copy in states:
        copy.start()
    weights = lambda i, slot: fetch_side_by_side([wg, wu], w_s, wsem, i, slot, wide)
    for copy in weights(0, 0):
        copy.start()
    for copy in states:
        copy.wait()
    for copy in weights(1, 1):
        copy.start()
    places = [pl.multiple_of(c * half, half) for c in (core(), 1 - core())]
    gains = [lambda place=place: gain_ref[:, pl.ds(place, half)].astype(F32) for place in places]
    norm_rows([h_s.at[0], h_s.at[1]], gains, b_s, places, rows, 2 * half)
    end_greeting()
    ride = Ride(given, [h_s.at[0], h_s.at[1], rest[0]], *made, rest[1]) if riding else None

    def body(i, _):
        slot = lax.rem(i, 2)
        for copy in weights(i, slot):
            copy.wait()
        both = dot(b_s[...], w_s[slot])
        hid_s[:, pl.ds(pl.multiple_of(i * wide, HEAD), wide)] = (jax.nn.silu(both[:, :wide]) * both[:, wide:]).astype(BF)

        @pl.when(i + 2 < steps)
        def _():
            for copy in weights(i + 2, slot):
                copy.start()

        @pl.when(i >= steps - 2)
        def _():
            j = i - steps + 2
            fetch(wd, wd_s, wdsem, block_column(j, n), j, wd_s.shape[2]).start()

        if riding:
            pl.when(i == 2)(ride.start)
            pl.when(i == 5)(ride.work)
        return 0

    lax.fori_loop(0, steps, body, 0)
    project(hid_s, wd, wd_s, wdsem, out_hbm, out_s, osem, send_s, recv_s, ssem, rsem, n)
    if riding:
        ride.end()


def mlp_half(hm, ht, first, rows, gain, wg, wu, wd, dep, ident, ride=(), wide=384, n=5):
    half = hm.shape[1]
    width, own = wg.shape
    bn = half // n
    shape = jax.ShapeDtypeStruct((rows, half), BF)
    return pl.pallas_call(
        functools.partial(mlp_kernel, first=first, n=n, riding=bool(ride)),
        in_specs=[ANY, ANY, pl.BlockSpec(memory_space=pltpu.VMEM), ANY, ANY, ANY, ANY, *[ANY] * len(ride)],
        out_specs=[ANY] * (3 if ride else 1),
        out_shape=[shape] * (3 if ride else 1),
        scratch_shapes=[pltpu.VMEM((2, rows, half), BF), pltpu.VMEM((rows, width), BF), pltpu.VMEM((2, width, 2 * wide), BF),
                        pltpu.VMEM((rows, own), BF), pltpu.VMEM((2, own, bn), BF), pltpu.VMEM((2, rows, bn), BF),
                        pltpu.VMEM((n, rows, bn), BF), pltpu.VMEM((n, rows, bn), BF), pltpu.SemaphoreType.DMA((2,)), pltpu.SemaphoreType.DMA((2, 2)),
                        pltpu.SemaphoreType.DMA((2,)), pltpu.SemaphoreType.DMA((2,)), pltpu.SemaphoreType.DMA((n,)), pltpu.SemaphoreType.DMA((n,)),
                        *([pltpu.VMEM((rows, half), BF), pltpu.SemaphoreType.DMA((6,))] if ride else [])],
        compiler_params=pltpu.CompilerParams(vmem_limit_bytes=VMEM, collective_id=ident, has_side_effects=True),
        cost_estimate=pl.CostEstimate(flops=6 * rows * width * own, bytes_accessed=6 * width * own, transcendentals=0),
        name="mlp_half",
    )(hm, ht, gain, wg, wu, wd, dep, *ride)


def finish_kernel(h_ref, one_ref, two_ref, *rest):
    y_ref, half_ref = rest[-2:]
    y_ref[...] = half_ref[...] = (h_ref[...].astype(F32) + (one_ref[...].astype(F32) + two_ref[...].astype(F32))).astype(BF)


def finished(h, first, at, terms, y, total, dep, block=256):
    rows, half = terms[0].shape
    own = pl.BlockSpec((block, half), lambda i: (i, 0))
    given = [dep] if y is None else [dep, y]
    return pl.pallas_call(
        finish_kernel,
        grid=(rows // block,),
        in_specs=[pl.BlockSpec((block, half), lambda i: (first // block + i, 0)), own, own] + [ANY] * len(given),
        out_specs=[pl.BlockSpec((block, half), lambda i: (at // block + i, core())), own],
        out_shape=[jax.ShapeDtypeStruct((total, 2 * half), BF), jax.ShapeDtypeStruct((rows, half), BF)],
        input_output_aliases={} if y is None else {4: 0},
        compiler_params=pltpu.CompilerParams(dimension_semantics=("arbitrary",)),
        cost_estimate=pl.CostEstimate(flops=10**9, bytes_accessed=10 * rows * half, transcendentals=0),
        name="finished",
    )(h, *terms, *given)


def place_kernel(t_ref, y_in, y_ref):
    y_ref[...] = t_ref[...]


def placed(theirs, y, at, block=256):
    rows, half = theirs.shape
    return pl.pallas_call(
        place_kernel,
        grid=(rows // block,),
        in_specs=[pl.BlockSpec((block, half), lambda i: (i, 0)), ANY],
        out_specs=pl.BlockSpec((block, half), lambda i: (at // block + i, 1 - core())),
        out_shape=jax.ShapeDtypeStruct(y.shape, BF),
        input_output_aliases={1: 0},
        compiler_params=pltpu.CompilerParams(dimension_semantics=("arbitrary",)),
        cost_estimate=pl.CostEstimate(flops=10**9, bytes_accessed=4 * rows * half, transcendentals=0),
        name="placed",
    )(theirs, y)


def solution(mesh):
    def layer(x, gain_a, wq, wk, wv, wo, gain_m, w_gate, w_up, w_down):
        batch, rows, d = x.shape
        x = x.reshape(batch * rows, d)
        gain_a, gain_m = gain_a.reshape(1, d), gain_m.reshape(1, d)
        half = HEAD // 2
        angle = jnp.arange(rows, dtype=F32)[:, None] * THETA ** (-jnp.arange(half, dtype=F32) / half)
        cos, sin = jnp.cos(angle), jnp.sin(angle)
        cos, sin = jnp.concatenate([cos, cos], 1), jnp.concatenate([-sin, sin], 1)

        def swap(t, pairs):
            return lax.ppermute(t, "tp", pairs)

        def kernel(call, *args, **kwargs):
            first, *more = call(*args, **kwargs)
            return (first, swap(first, CHIPS)), *more

        pair = (gain_a,)
        terms, h = [], []
        for s in range(batch):
            ride = terms[0] if s == batch - 1 else ()
            pair, own, *made = kernel(attend_half, x, s, rows, gain_a, cos, sin, wq, wk, wv, wo, pair[0], ride=ride)
            terms.append((own, *pair))
        h.append(made)

        got = []
        for s in range(batch):
            ride = terms[s + 1] if s + 1 < batch else ()
            pieces = 1 if ride else 2
            for p in range(pieces):
                size = rows // pieces
                pair, *made = kernel(mlp_half, *h[s], p * size, size, gain_m, w_gate, w_up, w_down, pair[0], batch + p + (not ride), ride=ride)
                got.append((s, p * size, pair))
            h.append(made)

        y, sent = None, []
        for s, first, pair in got:
            at = s * rows + first
            y, half = finished(h[s][0], first, at, pair, y, batch * rows, got[-1][2][0])
            sent.append((at, swap(half, CORES)))
            if len(sent) > 1:
                y = placed(sent[-2][1], y, sent[-2][0])
        y = placed(sent[-1][1], y, sent[-1][0])
        return y.reshape(batch, rows, d)

    tokens, whole, columns, rows_of = P("dp", None, None), P(None), P(None, "tp"), P("tp", None)
    return jax.shard_map(
        layer,
        mesh=mesh,
        in_specs=(tokens, whole, columns, columns, columns, rows_of, whole, columns, columns, rows_of),
        out_specs=tokens,
        check_vma=False,
    )
```

```python
import functools

import jax
import jax.numpy as jnp
from jax import lax
from jax.experimental import pallas as pl
from jax.experimental.pallas import tpu as pltpu
from jax.sharding import PartitionSpec as P

HEAD = 128
THETA = 10000
LOG2E = 1.4426950408889634
MESH = pl.DeviceIdType.MESH
BF, F32 = jnp.bfloat16, jnp.float32
VMEM = 67043328
PARTS = 4
DEEP = {3: 2, 0: 3}
CORES = [(0, 1), (1, 0), (2, 3), (3, 2)]
CHIPS = [(0, 2), (2, 0), (1, 3), (3, 1)]
ANY = pl.BlockSpec(memory_space=pl.ANY)


def dot(a, b):
    return jnp.dot(a, b, preferred_element_type=F32)


def core():
    return lax.rem(lax.axis_index("tp"), 2)


def start_greeting():
    pl.semaphore_signal(pltpu.get_barrier_semaphore(), inc=1, device_id=partner(), device_id_type=MESH)


def end_greeting():
    pl.semaphore_wait(pltpu.get_barrier_semaphore(), 1)


def partner():
    me = lax.axis_index("tp")
    return lax.axis_index("dp"), me + 1 - 2 * lax.rem(me, 2)


def sending(send_s, recv_s, ssem, rsem, j):
    return pltpu.make_async_remote_copy(
        src_ref=send_s.at[j], dst_ref=recv_s.at[j], send_sem=ssem.at[j], recv_sem=rsem.at[j], device_id=partner(), device_id_type=MESH
    )


def block_column(j, n):
    c = core()
    return jnp.where(j < n, (1 - c) * n + j, c * n + j - n)


def project(lhs_s, w_hbm, w_s, wsem, out_hbm, out_s, osem, term_s, send_s, recv_s, ssem, rsem, n):
    deep, _, bn = w_s.shape

    def body(j, _):
        slot = lax.rem(j, deep)
        fetch(w_hbm, w_s, wsem, block_column(j, n), slot, bn).wait()
        term_s[...] = dot(lhs_s[...], w_s[slot])

        @pl.when(j + deep < 2 * n)
        def _():
            fetch(w_hbm, w_s, wsem, block_column(j + deep, n), slot, bn).start()

        @pl.when(j < n)
        def _():
            send_s[j] = term_s[...].astype(BF)
            sending(send_s, recv_s, ssem, rsem, j).start()

        @pl.when(j >= n)
        def _():
            at, side = j - n, lax.rem(j - n, 2)
            sending(send_s, recv_s, ssem, rsem, at).wait_recv()

            @pl.when(at >= 2)
            def _():
                give(out_s, out_hbm, osem, at - 2, side, bn).wait()

            out_s[side] = (term_s[...] + recv_s[at].astype(F32)).astype(BF)
            give(out_s, out_hbm, osem, at, side, bn).start()

        return 0

    lax.fori_loop(0, 2 * n, body, 0)
    for j in range(n):
        sending(send_s, recv_s, ssem, rsem, j).wait_send()
    for j in range(max(n - 2, 0), n):
        give(out_s, out_hbm, osem, j, j % 2, bn).wait()


def fetch(hbm, vmem, sem, block, slot, bn):
    return pltpu.make_async_copy(hbm.at[:, pl.ds(pl.multiple_of(block * bn, bn), bn)], vmem.at[slot], sem.at[slot])


def give(vmem, hbm, sem, block, slot, bn):
    return pltpu.make_async_copy(vmem.at[slot], hbm.at[:, pl.ds(pl.multiple_of(block * bn, bn), bn)], sem.at[slot])


def fetch_side_by_side(refs, vmem, sem, block, slot, wide):
    at = pl.ds(pl.multiple_of(block * wide, HEAD), wide)
    return [pltpu.make_async_copy(r.at[:, at], vmem.at[slot, :, k * wide : (k + 1) * wide], sem.at[slot, k]) for k, r in enumerate(refs)]


class Ride:
    def __init__(self, terms, bufs, mine, theirs, sems):
        self.loads = [pltpu.make_async_copy(t, b, sems.at[k]) for k, (t, b) in enumerate(zip(terms, bufs))]
        self.bufs = bufs
        self.keep = pltpu.make_async_copy(bufs[2], mine, sems.at[3])
        self.send = pltpu.make_async_remote_copy(
            src_ref=bufs[2], dst_ref=theirs, send_sem=sems.at[4], recv_sem=sems.at[5], device_id=partner(), device_id_type=MESH
        )

    def start(self):
        for copy in self.loads:
            copy.start()

    def work(self, step=16):
        for copy in self.loads:
            copy.wait()
        base, one, two = self.bufs

        def body(r, _):
            at = pl.ds(pl.multiple_of(r * step, step), step)
            two[at, :] = (base[at, :].astype(F32) + (one[at, :].astype(F32) + two[at, :].astype(F32))).astype(BF)
            return 0

        lax.fori_loop(0, two.shape[0] // step, body, 0, unroll=2)
        self.keep.start()
        self.send.start()

    def end(self):
        self.keep.wait()
        self.send.wait()


def norm_rows(parts, gains, out_ref, places, first, rows, width, step=16):
    def body(r, _):
        at = pl.ds(pl.multiple_of(first + r * step, step), step)
        wide = [p[at, :].astype(F32) for p in parts]
        total = sum(jnp.sum(w * w, -1, keepdims=True) for w in wide)
        scale = lax.rsqrt(total * (1.0 / width) + 1e-6)
        for w, g, place in zip(wide, gains, places):
            out_ref[at, pl.ds(place, w.shape[1])] = (w * scale * g()).astype(BF)
        return 0

    lax.fori_loop(0, rows // step, body, 0, unroll=4)


def attend_kernel(x_hbm, gain_ref, cos_ref, sin_ref, wq, wk, wv, wo, dep, *rest, s, n, riding):
    given, rest = (rest[:3], rest[3:]) if riding else ((), rest)
    (out_hbm, half_hbm), rest = rest[:2], rest[2:]
    made, rest = (rest[:2], rest[2:]) if riding else ((), rest)
    x_s, a_s, w_s, qkv_s, seen_s, wo_s, out_s, term_s, send_s, recv_s, xsem, wsem, wosem, osem, ssem, rsem, *rest = rest
    rows, width = x_s.shape
    half = width // 2
    own, wide = seen_s.shape[1], w_s.shape[2] // 3
    steps, bq = own // wide, rows // 2
    start_greeting()
    part = rows // PARTS
    states = [pltpu.make_async_copy(x_hbm.at[pl.ds(s * rows + k * part, part)], x_s.at[pl.ds(k * part, part)], xsem.at[k]) for k in range(PARTS)]
    for copy in states:
        copy.start()
    weights = lambda i, slot: fetch_side_by_side([wq, wk, wv], w_s, wsem, i, slot, wide)
    for k, copy in enumerate(states):
        copy.wait()
        if k == 0:
            for load in weights(0, 0):
                load.start()
        norm_rows([x_s], [lambda: gain_ref[...].astype(F32)[None]], a_s, [0], k * part, part, width)
    for copy in weights(1, 1):
        copy.start()
    keep = pltpu.make_async_copy(x_s.at[:, pl.ds(pl.multiple_of(core() * half, half), half)], half_hbm, xsem.at[PARTS])
    keep.start()
    end_greeting()
    ride = Ride(given, [x_s.at[:, :half], x_s.at[:, half:], rest[0]], *made, rest[1]) if riding else None
    if riding:
        keep.wait()

    def heads(slot):
        found = dot(a_s[...], w_s[slot])
        cos, sin = cos_ref[...], sin_ref[...]
        for k in range(3 * wide // HEAD):
            cols = slice(k * HEAD, (k + 1) * HEAD)
            t = found[:, cols].astype(BF)
            if k < 2 * wide // HEAD:
                t = t.astype(F32)
                t = (t * cos + pltpu.roll(t, HEAD // 2, 1) * sin).astype(BF)
            qkv_s[slot, :, cols] = t

    def attention(i, slot):
        e = HEAD**-0.5 * LOG2E
        hidden = lax.broadcasted_iota(jnp.int32, (bq, bq), 0) < lax.broadcasted_iota(jnp.int32, (bq, bq), 1)
        pieces = [(h, b) for h in range(wide // HEAD) for b in range(rows // bq)]
        part = lambda what, h: slice(what * wide + h * HEAD, what * wide + (h + 1) * HEAD)
        scores = []
        for h, b in pieces:
            q, k = qkv_s[slot, b * bq : (b + 1) * bq, part(0, h)], qkv_s[slot, : (b + 1) * bq, part(1, h)]
            scores.append(lax.dot_general(q, k, (((1,), (1,)), ((), ())), preferred_element_type=F32))
        weights = []
        for (h, b), t in zip(pieces, scores):
            last = jnp.where(hidden, -1e30, t[:, b * bq :])
            t = last if b == 0 else jnp.concatenate([t[:, : b * bq], last], 1)
            p = jnp.exp2((t - t.max(-1, keepdims=True)) * e)
            weights.append((p.astype(BF), p.sum(-1, keepdims=True)))
        for (h, b), (p, total) in zip(pieces, weights):
            o = dot(p, qkv_s[slot, : (b + 1) * bq, part(2, h)]) / total
            seen_s[b * bq : (b + 1) * bq, pl.ds(pl.multiple_of(i * wide + h * HEAD, HEAD), HEAD)] = o.astype(BF)

    def body(i, _):
        slot = lax.rem(i, 2)
        for copy in weights(i, slot):
            copy.wait()
        attention(jnp.maximum(i - 1, 0), 1 - slot)
        heads(slot)

        @pl.when(i + 2 < steps)
        def _():
            for copy in weights(i + 2, slot):
                copy.start()

        @pl.when(i >= steps - 2)
        def _():
            j = i - steps + 2
            fetch(wo, wo_s, wosem, block_column(j, n), j, wo_s.shape[2]).start()

        if riding:
            pl.when(i == 0)(ride.start)
            pl.when(i == 3)(ride.work)
        return 0

    qkv_s[1] = jnp.zeros_like(qkv_s[1])
    lax.fori_loop(0, steps, body, 0)
    attention(steps - 1, (steps - 1) % 2)
    project(seen_s, wo, wo_s, wosem, out_hbm, out_s, osem, term_s, send_s, recv_s, ssem, rsem, n)
    if riding:
        ride.end()
    else:
        keep.wait()


def attend_half(x, s, rows, gain, cos, sin, wq, wk, wv, wo, dep, ride=(), wide=256, n=2):
    width, own = wq.shape
    bn = width // 2 // n
    half = jax.ShapeDtypeStruct((rows, width // 2), BF)
    whole = pl.BlockSpec(memory_space=pltpu.VMEM)
    return pl.pallas_call(
        functools.partial(attend_kernel, s=s, n=n, riding=bool(ride)),
        in_specs=[ANY, whole, whole, whole, ANY, ANY, ANY, ANY, ANY, *[ANY] * len(ride)],
        out_specs=[ANY] * (4 if ride else 2),
        out_shape=[half] * (4 if ride else 2),
        scratch_shapes=[pltpu.VMEM((rows, width), BF), pltpu.VMEM((rows, width), BF), pltpu.VMEM((2, width, 3 * wide), BF), pltpu.VMEM((2, rows, 3 * wide), BF),
                        pltpu.VMEM((rows, own), BF), pltpu.VMEM((2, own, bn), BF), pltpu.VMEM((2, rows, bn), BF), pltpu.VMEM((rows, bn), F32),
                        pltpu.VMEM((n, rows, bn), BF), pltpu.VMEM((n, rows, bn), BF), pltpu.SemaphoreType.DMA((PARTS + 1,)), pltpu.SemaphoreType.DMA((2, 3)),
                        pltpu.SemaphoreType.DMA((2,)), pltpu.SemaphoreType.DMA((2,)), pltpu.SemaphoreType.DMA((n,)), pltpu.SemaphoreType.DMA((n,)),
                        *([pltpu.VMEM((rows, width // 2), BF), pltpu.SemaphoreType.DMA((6,))] if ride else [])],
        compiler_params=pltpu.CompilerParams(vmem_limit_bytes=VMEM, collective_id=s, has_side_effects=True),
        cost_estimate=pl.CostEstimate(flops=8 * rows * width * own, bytes_accessed=8 * width * own, transcendentals=0),
        name="attend_half",
    )(x, gain, cos, sin, wq, wk, wv, wo, dep, *ride)


def mlp_kernel(hm, ht, gain_ref, wg, wu, wd, dep, *rest, first, n, riding):
    given, rest = (rest[:3], rest[3:]) if riding else ((), rest)
    out_hbm, *rest = rest
    made, rest = (rest[:2], rest[2:]) if riding else ((), rest)
    h_s, b_s, w_s, hid_s, wd_s, out_s, term_s, send_s, recv_s, hsem, wsem, wdsem, osem, ssem, rsem, *rest = rest
    rows, half = h_s.shape[1:]
    own, wide = hid_s.shape[1], w_s.shape[2] // 2
    steps = own // wide
    start_greeting()
    part = rows // PARTS
    states = [[pltpu.make_async_copy(r.at[pl.ds(first + k * part, part)], h_s.at[e, pl.ds(k * part, part)], hsem.at[k, e]) for e, r in enumerate((hm, ht))]
              for k in range(PARTS)]
    for pair in states:
        for copy in pair:
            copy.start()
    weights = lambda i, slot: fetch_side_by_side([wg, wu], w_s, wsem, i, slot, wide)
    places = [pl.multiple_of(c * half, half) for c in (core(), 1 - core())]
    gains = [lambda place=place: gain_ref[pl.ds(place, half)].astype(F32)[None] for place in places]
    for k, pair in enumerate(states):
        for copy in pair:
            copy.wait()
        if k == 0:
            for copy in weights(0, 0):
                copy.start()
        norm_rows([h_s.at[0], h_s.at[1]], gains, b_s, places, k * part, part, 2 * half)
    deep = w_s.shape[0]
    for i in range(1, deep):
        for copy in weights(i, i):
            copy.start()
    end_greeting()
    ride = Ride(given, [h_s.at[0], h_s.at[1], rest[0]], *made, rest[1]) if riding else None

    def body(i, _):
        slot = lax.rem(i, deep)
        for copy in weights(i, slot):
            copy.wait()
        both = dot(b_s[...], w_s[slot])
        hid_s[:, pl.ds(pl.multiple_of(i * wide, HEAD), wide)] = (jax.nn.silu(both[:, :wide]) * both[:, wide:]).astype(BF)

        @pl.when(i + deep < steps)
        def _():
            for copy in weights(i + deep, slot):
                copy.start()

        @pl.when(i >= steps - wd_s.shape[0])
        def _():
            j = i - steps + wd_s.shape[0]
            fetch(wd, wd_s, wdsem, block_column(j, n), j, wd_s.shape[2]).start()

        if riding:
            pl.when(i == 2)(ride.start)
            pl.when(i == 5)(ride.work)
        return 0

    lax.fori_loop(0, steps, body, 0)
    project(hid_s, wd, wd_s, wdsem, out_hbm, out_s, osem, term_s, send_s, recv_s, ssem, rsem, n)
    if riding:
        ride.end()


def mlp_half(hm, ht, first, rows, gain, wg, wu, wd, dep, ident, ride=(), wide=384, n=5, deep=2):
    half = hm.shape[1]
    width, own = wg.shape
    bn = half // n
    shape = jax.ShapeDtypeStruct((rows, half), BF)
    return pl.pallas_call(
        functools.partial(mlp_kernel, first=first, n=n, riding=bool(ride)),
        in_specs=[ANY, ANY, pl.BlockSpec(memory_space=pltpu.VMEM), ANY, ANY, ANY, ANY, *[ANY] * len(ride)],
        out_specs=[ANY] * (3 if ride else 1),
        out_shape=[shape] * (3 if ride else 1),
        scratch_shapes=[pltpu.VMEM((2, rows, half), BF), pltpu.VMEM((rows, width), BF), pltpu.VMEM((deep, width, 2 * wide), BF),
                        pltpu.VMEM((rows, own), BF), pltpu.VMEM((deep, own, bn), BF), pltpu.VMEM((2, rows, bn), BF), pltpu.VMEM((rows, bn), F32),
                        pltpu.VMEM((n, rows, bn), BF), pltpu.VMEM((n, rows, bn), BF), pltpu.SemaphoreType.DMA((PARTS, 2)), pltpu.SemaphoreType.DMA((deep, 2)),
                        pltpu.SemaphoreType.DMA((deep,)), pltpu.SemaphoreType.DMA((2,)), pltpu.SemaphoreType.DMA((n,)), pltpu.SemaphoreType.DMA((n,)),
                        *([pltpu.VMEM((rows, half), BF), pltpu.SemaphoreType.DMA((6,))] if ride else [])],
        compiler_params=pltpu.CompilerParams(vmem_limit_bytes=VMEM, collective_id=ident, has_side_effects=True),
        cost_estimate=pl.CostEstimate(flops=6 * rows * width * own, bytes_accessed=6 * width * own, transcendentals=0),
        name="mlp_half",
    )(hm, ht, gain, wg, wu, wd, dep, *ride)


def finish_kernel(h_ref, one_ref, two_ref, *rest):
    y_ref, half_ref = rest[-2:]
    y_ref[...] = half_ref[...] = (h_ref[...].astype(F32) + (one_ref[...].astype(F32) + two_ref[...].astype(F32))).astype(BF)


def finished(h, first, at, terms, y, total, dep, block=256):
    rows, half = terms[0].shape
    own = pl.BlockSpec((block, half), lambda i: (i, 0))
    given = [dep] if y is None else [dep, y]
    return pl.pallas_call(
        finish_kernel,
        grid=(rows // block,),
        in_specs=[pl.BlockSpec((block, half), lambda i: (first // block + i, 0)), own, own] + [ANY] * len(given),
        out_specs=[pl.BlockSpec((block, half), lambda i: (at // block + i, core())), own],
        out_shape=[jax.ShapeDtypeStruct((total, 2 * half), BF), jax.ShapeDtypeStruct((rows, half), BF)],
        input_output_aliases={} if y is None else {4: 0},
        compiler_params=pltpu.CompilerParams(dimension_semantics=("arbitrary",), vmem_limit_bytes=VMEM),
        cost_estimate=pl.CostEstimate(flops=10**9, bytes_accessed=10 * rows * half, transcendentals=0),
        name="finished",
    )(h, *terms, *given)


def place_kernel(t_ref, y_in, y_ref):
    y_ref[...] = t_ref[...]


def placed(theirs, y, at, block=256):
    rows, half = theirs.shape
    return pl.pallas_call(
        place_kernel,
        grid=(rows // block,),
        in_specs=[pl.BlockSpec((block, half), lambda i: (i, 0)), ANY],
        out_specs=pl.BlockSpec((block, half), lambda i: (at // block + i, 1 - core())),
        out_shape=jax.ShapeDtypeStruct(y.shape, BF),
        input_output_aliases={1: 0},
        compiler_params=pltpu.CompilerParams(dimension_semantics=("arbitrary",), vmem_limit_bytes=VMEM),
        cost_estimate=pl.CostEstimate(flops=10**9, bytes_accessed=4 * rows * half, transcendentals=0),
        name="placed",
    )(theirs, y)


def solution(mesh):
    def layer(x, gain_a, wq, wk, wv, wo, gain_m, w_gate, w_up, w_down):
        batch, rows, d = x.shape
        x = x.reshape(batch * rows, d)
        half = HEAD // 2
        angle = jnp.arange(rows, dtype=F32)[:, None] * THETA ** (-jnp.arange(half, dtype=F32) / half)
        cos, sin = jnp.cos(angle), jnp.sin(angle)
        cos, sin = jnp.concatenate([cos, cos], 1), jnp.concatenate([-sin, sin], 1)

        def swap(t, pairs):
            return lax.ppermute(t, "tp", pairs)

        def kernel(call, *args, **kwargs):
            first, *more = call(*args, **kwargs)
            return (first, swap(first, CHIPS)), *more

        pair = (gain_a,)
        terms, h = [], []
        for s in range(batch):
            ride = terms[0] if s == batch - 1 else ()
            pair, own, *made = kernel(attend_half, x, s, rows, gain_a, cos, sin, wq, wk, wv, wo, pair[0], ride=ride)
            terms.append((own, *pair))
        h.append(made)

        got = []
        for s in range(batch):
            ride = terms[s + 1] if s + 1 < batch else ()
            pieces = 1 if ride else 2
            for p in range(pieces):
                size = rows // pieces
                pair, *made = kernel(mlp_half, *h[s], p * size, size, gain_m, w_gate, w_up, w_down, pair[0], batch + p + (not ride), ride=ride, deep=DEEP[len(ride)])
                got.append((s, p * size, pair))
            h.append(made)

        y, sent = None, []
        for s, first, pair in got:
            at = s * rows + first
            y, half = finished(h[s][0], first, at, pair, y, batch * rows, got[-1][2][0])
            sent.append((at, swap(half, CORES)))
            if len(sent) > 1:
                y = placed(sent[-2][1], y, sent[-2][0])
        y = placed(sent[-1][1], y, sent[-1][0])
        return y.reshape(batch, rows, d)

    tokens, whole, columns, rows_of = P("dp", None, None), P(None), P(None, "tp"), P("tp", None)
    return jax.shard_map(
        layer,
        mesh=mesh,
        in_specs=(tokens, whole, columns, columns, columns, rows_of, whole, columns, columns, rows_of),
        out_specs=tokens,
        check_vma=False,
    )
```

```python
import functools

import jax
import jax.numpy as jnp
import numpy as np
from jax import lax
from jax.experimental import pallas as pl
from jax.experimental.pallas import tpu as pltpu
from jax.sharding import PartitionSpec as P

HEAD = 128
THETA = 10000
LOG2E = 1.4426950408889634
MESH = pl.DeviceIdType.MESH
BF, F32 = jnp.bfloat16, jnp.float32
VMEM = 67043328
PARTS = 4
DEEP = {3: 2, 0: 3}
CORES = [(0, 1), (1, 0), (2, 3), (3, 2)]
CHIPS = [(0, 2), (2, 0), (1, 3), (3, 1)]
ANY = pl.BlockSpec(memory_space=pl.ANY)


def dot(a, b):
    return jnp.dot(a, b, preferred_element_type=F32)


def core():
    return lax.rem(lax.axis_index("tp"), 2)


def start_greeting():
    pl.semaphore_signal(pltpu.get_barrier_semaphore(), inc=1, device_id=partner(), device_id_type=MESH)


def end_greeting():
    pl.semaphore_wait(pltpu.get_barrier_semaphore(), 1)


def partner():
    me = lax.axis_index("tp")
    return lax.axis_index("dp"), me + 1 - 2 * lax.rem(me, 2)


def sending(send_s, recv_s, ssem, rsem, j):
    return pltpu.make_async_remote_copy(
        src_ref=send_s.at[j], dst_ref=recv_s.at[j], send_sem=ssem.at[j], recv_sem=rsem.at[j], device_id=partner(), device_id_type=MESH
    )


def block_column(j, n):
    c = core()
    return jnp.where(j < n, (1 - c) * n + j, c * n + j - n)


def project(lhs_s, w_hbm, w_s, wsem, out_hbm, out_s, osem, term_s, send_s, recv_s, ssem, rsem, n):
    deep, _, bn = w_s.shape

    def body(j, _):
        slot = lax.rem(j, deep)
        fetch(w_hbm, w_s, wsem, block_column(j, n), slot, bn).wait()
        term_s[...] = dot(lhs_s[...], w_s[slot])

        @pl.when(j + deep < 2 * n)
        def _():
            fetch(w_hbm, w_s, wsem, block_column(j + deep, n), slot, bn).start()

        @pl.when(j < n)
        def _():
            send_s[j] = term_s[...].astype(BF)
            sending(send_s, recv_s, ssem, rsem, j).start()

        @pl.when(j >= n)
        def _():
            at, side = j - n, lax.rem(j - n, 2)
            sending(send_s, recv_s, ssem, rsem, at).wait_recv()

            @pl.when(at >= 2)
            def _():
                give(out_s, out_hbm, osem, at - 2, side, bn).wait()

            out_s[side] = (term_s[...] + recv_s[at].astype(F32)).astype(BF)
            give(out_s, out_hbm, osem, at, side, bn).start()

        return 0

    lax.fori_loop(0, 2 * n, body, 0)
    for j in range(n):
        sending(send_s, recv_s, ssem, rsem, j).wait_send()
    for j in range(max(n - 2, 0), n):
        give(out_s, out_hbm, osem, j, j % 2, bn).wait()


def fetch(hbm, vmem, sem, block, slot, bn):
    return pltpu.make_async_copy(hbm.at[:, pl.ds(pl.multiple_of(block * bn, bn), bn)], vmem.at[slot], sem.at[slot])


def give(vmem, hbm, sem, block, slot, bn):
    return pltpu.make_async_copy(vmem.at[slot], hbm.at[:, pl.ds(pl.multiple_of(block * bn, bn), bn)], sem.at[slot])


def fetch_side_by_side(refs, vmem, sem, block, slot, wide):
    at = pl.ds(pl.multiple_of(block * wide, HEAD), wide)
    return [pltpu.make_async_copy(r.at[:, at], vmem.at[slot, :, k * wide : (k + 1) * wide], sem.at[slot, k]) for k, r in enumerate(refs)]


class Ride:
    def __init__(self, terms, bufs, mine, theirs, sems):
        self.loads = [pltpu.make_async_copy(t, b, sems.at[k]) for k, (t, b) in enumerate(zip(terms, bufs))]
        self.bufs = bufs
        self.keep = pltpu.make_async_copy(bufs[2], mine, sems.at[3])
        self.send = pltpu.make_async_remote_copy(
            src_ref=bufs[2], dst_ref=theirs, send_sem=sems.at[4], recv_sem=sems.at[5], device_id=partner(), device_id_type=MESH
        )

    def start(self):
        for copy in self.loads:
            copy.start()

    def work(self, step=16):
        for copy in self.loads:
            copy.wait()
        base, one, two = self.bufs

        def body(r, _):
            at = pl.ds(pl.multiple_of(r * step, step), step)
            two[at, :] = (base[at, :].astype(F32) + (one[at, :].astype(F32) + two[at, :].astype(F32))).astype(BF)
            return 0

        lax.fori_loop(0, two.shape[0] // step, body, 0, unroll=2)
        self.keep.start()
        self.send.start()

    def end(self):
        self.keep.wait()
        self.send.wait()


def norm_rows(parts, gains, out_ref, places, first, rows, width, step=16):
    def body(r, _):
        at = pl.ds(pl.multiple_of(first + r * step, step), step)
        wide = [p[at, :].astype(F32) for p in parts]
        total = sum(jnp.sum(w * w, -1, keepdims=True) for w in wide)
        scale = lax.rsqrt(total * (1.0 / width) + 1e-6)
        for w, g, place in zip(wide, gains, places):
            out_ref[at, pl.ds(place, w.shape[1])] = (w * scale * g()).astype(BF)
        return 0

    lax.fori_loop(0, rows // step, body, 0, unroll=4)


def attend_kernel(x_hbm, gain_ref, cos_ref, sin_ref, wq, wk, wv, wo, dep, *rest, s, n, riding):
    given, rest = (rest[:3], rest[3:]) if riding else ((), rest)
    (out_hbm, half_hbm), rest = rest[:2], rest[2:]
    made, rest = (rest[:2], rest[2:]) if riding else ((), rest)
    x_s, a_s, w_s, qkv_s, seen_s, wo_s, out_s, term_s, send_s, recv_s, xsem, wsem, wosem, osem, ssem, rsem, *rest = rest
    rows, width = x_s.shape
    half = width // 2
    own, wide = seen_s.shape[1], w_s.shape[2] // 3
    steps, bq = own // wide, rows // 2
    start_greeting()
    part = rows // PARTS
    states = lambda k: pltpu.make_async_copy(x_hbm.at[pl.ds(s * rows + k * part, part)], x_s.at[pl.ds(k * part, part)], xsem.at[k])
    for k in range(PARTS):
        states(k).start()
    weights = lambda i, slot: fetch_side_by_side([wq, wk, wv], w_s, wsem, i, slot, wide)

    def arrive(k, _):
        states(k).wait()

        @pl.when(k == 0)
        def _():
            for load in weights(0, 0):
                load.start()

        norm_rows([x_s], [lambda: gain_ref[...].astype(F32)[None]], a_s, [0], k * part, part, width)
        return 0

    lax.fori_loop(0, PARTS, arrive, 0)
    for copy in weights(1, 1):
        copy.start()
    keep = pltpu.make_async_copy(x_s.at[:, pl.ds(pl.multiple_of(core() * half, half), half)], half_hbm, xsem.at[PARTS])
    keep.start()
    end_greeting()
    ride = Ride(given, [x_s.at[:, :half], x_s.at[:, half:], rest[0]], *made, rest[1]) if riding else None
    if riding:
        keep.wait()

    def heads(slot):
        found = dot(a_s[...], w_s[slot])
        cos, sin = cos_ref[...], sin_ref[...]
        for k in range(3 * wide // HEAD):
            cols = slice(k * HEAD, (k + 1) * HEAD)
            t = found[:, cols].astype(BF)
            if k < 2 * wide // HEAD:
                t = t.astype(F32)
                t = (t * cos + pltpu.roll(t, HEAD // 2, 1) * sin).astype(BF)
            qkv_s[slot, :, cols] = t

    def attention(i, slot):
        e = HEAD**-0.5 * LOG2E
        hidden = lax.broadcasted_iota(jnp.int32, (bq, bq), 0) < lax.broadcasted_iota(jnp.int32, (bq, bq), 1)
        pieces = [(h, b) for h in range(wide // HEAD) for b in range(rows // bq)]
        part = lambda what, h: slice(what * wide + h * HEAD, what * wide + (h + 1) * HEAD)
        scores = []
        for h, b in pieces:
            q, k = qkv_s[slot, b * bq : (b + 1) * bq, part(0, h)], qkv_s[slot, : (b + 1) * bq, part(1, h)]
            scores.append(lax.dot_general(q, k, (((1,), (1,)), ((), ())), preferred_element_type=F32))
        weights = []
        for (h, b), t in zip(pieces, scores):
            last = jnp.where(hidden, -1e30, t[:, b * bq :])
            t = last if b == 0 else jnp.concatenate([t[:, : b * bq], last], 1)
            p = jnp.exp2((t - t.max(-1, keepdims=True)) * e)
            weights.append((p.astype(BF), p.sum(-1, keepdims=True)))
        for (h, b), (p, total) in zip(pieces, weights):
            o = dot(p, qkv_s[slot, : (b + 1) * bq, part(2, h)]) / total
            seen_s[b * bq : (b + 1) * bq, pl.ds(pl.multiple_of(i * wide + h * HEAD, HEAD), HEAD)] = o.astype(BF)

    def body(i, _):
        slot = lax.rem(i, 2)
        for copy in weights(i, slot):
            copy.wait()
        attention(jnp.maximum(i - 1, 0), 1 - slot)
        heads(slot)

        @pl.when(i + 2 < steps)
        def _():
            for copy in weights(i + 2, slot):
                copy.start()

        @pl.when(i >= steps - 2)
        def _():
            j = i - steps + 2
            fetch(wo, wo_s, wosem, block_column(j, n), j, wo_s.shape[2]).start()

        if riding:
            pl.when(i == 0)(ride.start)
            pl.when(i == 3)(ride.work)
        return 0

    qkv_s[1] = jnp.zeros_like(qkv_s[1])
    lax.fori_loop(0, steps, body, 0)
    attention(steps - 1, (steps - 1) % 2)
    project(seen_s, wo, wo_s, wosem, out_hbm, out_s, osem, term_s, send_s, recv_s, ssem, rsem, n)
    if riding:
        ride.end()
    else:
        keep.wait()


def attend_half(x, s, rows, gain, cos, sin, wq, wk, wv, wo, dep, ride=(), wide=256, n=2):
    width, own = wq.shape
    bn = width // 2 // n
    half = jax.ShapeDtypeStruct((rows, width // 2), BF)
    whole = pl.BlockSpec(memory_space=pltpu.VMEM)
    return pl.pallas_call(
        functools.partial(attend_kernel, s=s, n=n, riding=bool(ride)),
        in_specs=[ANY, whole, whole, whole, ANY, ANY, ANY, ANY, ANY, *[ANY] * len(ride)],
        out_specs=[ANY] * (4 if ride else 2),
        out_shape=[half] * (4 if ride else 2),
        scratch_shapes=[pltpu.VMEM((rows, width), BF), pltpu.VMEM((rows, width), BF), pltpu.VMEM((2, width, 3 * wide), BF), pltpu.VMEM((2, rows, 3 * wide), BF),
                        pltpu.VMEM((rows, own), BF), pltpu.VMEM((2, own, bn), BF), pltpu.VMEM((2, rows, bn), BF), pltpu.VMEM((rows, bn), F32),
                        pltpu.VMEM((n, rows, bn), BF), pltpu.VMEM((n, rows, bn), BF), pltpu.SemaphoreType.DMA((PARTS + 1,)), pltpu.SemaphoreType.DMA((2, 3)),
                        pltpu.SemaphoreType.DMA((2,)), pltpu.SemaphoreType.DMA((2,)), pltpu.SemaphoreType.DMA((n,)), pltpu.SemaphoreType.DMA((n,)),
                        *([pltpu.VMEM((rows, width // 2), BF), pltpu.SemaphoreType.DMA((6,))] if ride else [])],
        compiler_params=pltpu.CompilerParams(vmem_limit_bytes=VMEM, collective_id=s, has_side_effects=True),
        cost_estimate=pl.CostEstimate(flops=8 * rows * width * own, bytes_accessed=8 * width * own, transcendentals=0),
        name="attend_half",
    )(x, gain, cos, sin, wq, wk, wv, wo, dep, *ride)


def mlp_kernel(hm, ht, gain_ref, wg, wu, wd, dep, *rest, first, n, riding):
    given, rest = (rest[:3], rest[3:]) if riding else ((), rest)
    out_hbm, *rest = rest
    made, rest = (rest[:2], rest[2:]) if riding else ((), rest)
    h_s, b_s, w_s, hid_s, wd_s, out_s, term_s, send_s, recv_s, hsem, wsem, wdsem, osem, ssem, rsem, *rest = rest
    rows, half = h_s.shape[1:]
    own, wide = hid_s.shape[1], w_s.shape[2] // 2
    steps = own // wide
    start_greeting()
    part = rows // PARTS
    states = lambda k: [pltpu.make_async_copy(r.at[pl.ds(first + k * part, part)], h_s.at[e, pl.ds(k * part, part)], hsem.at[k, e]) for e, r in enumerate((hm, ht))]
    for k in range(PARTS):
        for copy in states(k):
            copy.start()
    weights = lambda i, slot: fetch_side_by_side([wg, wu], w_s, wsem, i, slot, wide)
    places = [pl.multiple_of(c * half, half) for c in (core(), 1 - core())]
    gains = [lambda place=place: gain_ref[pl.ds(place, half)].astype(F32)[None] for place in places]

    def arrive(k, _):
        for copy in states(k):
            copy.wait()

        @pl.when(k == 0)
        def _():
            for copy in weights(0, 0):
                copy.start()

        norm_rows([h_s.at[0], h_s.at[1]], gains, b_s, places, k * part, part, 2 * half)
        return 0

    lax.fori_loop(0, PARTS, arrive, 0)
    deep = w_s.shape[0]
    for i in range(1, deep):
        for copy in weights(i, i):
            copy.start()
    end_greeting()
    ride = Ride(given, [h_s.at[0], h_s.at[1], rest[0]], *made, rest[1]) if riding else None

    def body(i, _):
        slot = lax.rem(i, deep)
        for copy in weights(i, slot):
            copy.wait()
        both = dot(b_s[...], w_s[slot])
        hid_s[:, pl.ds(pl.multiple_of(i * wide, HEAD), wide)] = (jax.nn.silu(both[:, :wide]) * both[:, wide:]).astype(BF)

        @pl.when(i + deep < steps)
        def _():
            for copy in weights(i + deep, slot):
                copy.start()

        @pl.when(i >= steps - wd_s.shape[0])
        def _():
            j = i - steps + wd_s.shape[0]
            fetch(wd, wd_s, wdsem, block_column(j, n), j, wd_s.shape[2]).start()

        if riding:
            pl.when(i == 2)(ride.start)
            pl.when(i == 5)(ride.work)
        return 0

    lax.fori_loop(0, steps, body, 0)
    project(hid_s, wd, wd_s, wdsem, out_hbm, out_s, osem, term_s, send_s, recv_s, ssem, rsem, n)
    if riding:
        ride.end()


def mlp_half(hm, ht, first, rows, gain, wg, wu, wd, dep, ident, ride=(), wide=384, n=5, deep=2):
    half = hm.shape[1]
    width, own = wg.shape
    bn = half // n
    shape = jax.ShapeDtypeStruct((rows, half), BF)
    return pl.pallas_call(
        functools.partial(mlp_kernel, first=first, n=n, riding=bool(ride)),
        in_specs=[ANY, ANY, pl.BlockSpec(memory_space=pltpu.VMEM), ANY, ANY, ANY, ANY, *[ANY] * len(ride)],
        out_specs=[ANY] * (3 if ride else 1),
        out_shape=[shape] * (3 if ride else 1),
        scratch_shapes=[pltpu.VMEM((2, rows, half), BF), pltpu.VMEM((rows, width), BF), pltpu.VMEM((deep, width, 2 * wide), BF),
                        pltpu.VMEM((rows, own), BF), pltpu.VMEM((deep, own, bn), BF), pltpu.VMEM((2, rows, bn), BF), pltpu.VMEM((rows, bn), F32),
                        pltpu.VMEM((n, rows, bn), BF), pltpu.VMEM((n, rows, bn), BF), pltpu.SemaphoreType.DMA((PARTS, 2)), pltpu.SemaphoreType.DMA((deep, 2)),
                        pltpu.SemaphoreType.DMA((deep,)), pltpu.SemaphoreType.DMA((2,)), pltpu.SemaphoreType.DMA((n,)), pltpu.SemaphoreType.DMA((n,)),
                        *([pltpu.VMEM((rows, half), BF), pltpu.SemaphoreType.DMA((6,))] if ride else [])],
        compiler_params=pltpu.CompilerParams(vmem_limit_bytes=VMEM, collective_id=ident, has_side_effects=True),
        cost_estimate=pl.CostEstimate(flops=6 * rows * width * own, bytes_accessed=6 * width * own, transcendentals=0),
        name="mlp_half",
    )(hm, ht, gain, wg, wu, wd, dep, *ride)


def finish_kernel(h_ref, one_ref, two_ref, *rest):
    y_ref, half_ref = rest[-2:]
    y_ref[...] = half_ref[...] = (h_ref[...].astype(F32) + (one_ref[...].astype(F32) + two_ref[...].astype(F32))).astype(BF)


def finished(h, first, at, terms, y, total, dep, block=256):
    rows, half = terms[0].shape
    block = min(block, rows // 2)
    own = pl.BlockSpec((block, half), lambda i: (i, 0))
    given = [dep] if y is None else [dep, y]
    return pl.pallas_call(
        finish_kernel,
        grid=(rows // block,),
        in_specs=[pl.BlockSpec((block, half), lambda i: (first // block + i, 0)), own, own] + [ANY] * len(given),
        out_specs=[pl.BlockSpec((block, half), lambda i: (at // block + i, core())), own],
        out_shape=[jax.ShapeDtypeStruct((total, 2 * half), BF), jax.ShapeDtypeStruct((rows, half), BF)],
        input_output_aliases={} if y is None else {4: 0},
        compiler_params=pltpu.CompilerParams(dimension_semantics=("arbitrary",), vmem_limit_bytes=VMEM),
        cost_estimate=pl.CostEstimate(flops=10**9, bytes_accessed=10 * rows * half, transcendentals=0),
        name="finished",
    )(h, *terms, *given)


def place_kernel(t_ref, y_in, y_ref):
    y_ref[...] = t_ref[...]


def placed(theirs, y, at, block=256):
    rows, half = theirs.shape
    block = min(block, rows // 2)
    return pl.pallas_call(
        place_kernel,
        grid=(rows // block,),
        in_specs=[pl.BlockSpec((block, half), lambda i: (i, 0)), ANY],
        out_specs=pl.BlockSpec((block, half), lambda i: (at // block + i, 1 - core())),
        out_shape=jax.ShapeDtypeStruct(y.shape, BF),
        input_output_aliases={1: 0},
        compiler_params=pltpu.CompilerParams(dimension_semantics=("arbitrary",), vmem_limit_bytes=VMEM),
        cost_estimate=pl.CostEstimate(flops=10**9, bytes_accessed=4 * rows * half, transcendentals=0),
        name="placed",
    )(theirs, y)


def tables(rows):
    half = HEAD // 2
    angle = np.arange(rows, dtype=np.float32)[:, None] * np.float32(THETA) ** (-np.arange(half, dtype=np.float32) / np.float32(half))
    cos, sin = np.cos(angle), np.sin(angle)
    return np.concatenate([cos, cos], 1), np.concatenate([-sin, sin], 1)


def solution(mesh):
    def layer(x, gain_a, wq, wk, wv, wo, gain_m, w_gate, w_up, w_down):
        batch, rows, d = x.shape
        x = x.reshape(batch * rows, d)
        cos, sin = tables(rows)

        def swap(t, pairs):
            return lax.ppermute(t, "tp", pairs)

        def kernel(call, *args, **kwargs):
            first, *more = call(*args, **kwargs)
            return (first, swap(first, CHIPS)), *more

        pair = (gain_a,)
        terms, h = [], []
        for s in range(batch):
            ride = terms[0] if s == batch - 1 else ()
            pair, own, *made = kernel(attend_half, x, s, rows, gain_a, cos, sin, wq, wk, wv, wo, pair[0], ride=ride)
            terms.append((own, *pair))
        h.append(made)

        got = []
        for s in range(batch):
            ride = terms[s + 1] if s + 1 < batch else ()
            pieces = 1 if ride else 2
            for p in range(pieces):
                size = rows // pieces
                pair, *made = kernel(mlp_half, *h[s], p * size, size, gain_m, w_gate, w_up, w_down, pair[0], batch + p + (not ride), ride=ride, deep=DEEP[len(ride)])
                got.append((s, p * size, pair))
            h.append(made)

        y, sent = None, []
        for s, first, pair in got:
            at = s * rows + first
            y, half = finished(h[s][0], first, at, pair, y, batch * rows, got[-1][2][0])
            sent.append((at, swap(half, CORES)))
            if len(sent) > 1:
                y = placed(sent[-2][1], y, sent[-2][0])
        y = placed(sent[-1][1], y, sent[-1][0])
        return y.reshape(batch, rows, d)

    tokens, whole, columns, rows_of = P("dp", None, None), P(None), P(None, "tp"), P("tp", None)
    return jax.shard_map(
        layer,
        mesh=mesh,
        in_specs=(tokens, whole, columns, columns, columns, rows_of, whole, columns, columns, rows_of),
        out_specs=tokens,
        check_vma=False,
    )
```
